256 devices in a mesh: seq: 32 (over z, y), head: 8 (over x, core).
Axes of the slice: x: 4, y: 4, z: 8, core: 2. Of those that a mesh axis runs over, the one named last changes fastest.
Arguments:
- queries: bfloat16 [32768, 12288], P(('seq', 'head')), may hold values from -8 to 8
- latent: bfloat16 [32768, 512], P(('seq', 'head')), may hold values from -6 to 6
- rope_keys: bfloat16 [32768, 64], P(('seq', 'head')), may hold values from -8 to 8
- key_weight: bfloat16 [512, 8192], P('seq', 'head'), may hold values from -0.25 to 0.25
- value_weight: bfloat16 [512, 8192], P('seq', 'head'), may hold values from -0.25 to 0.25
- doc_lengths: int32 [128], replicated, may hold values from 1 to 510, as said below
Outputs:
- attended: bfloat16 [32768, 8192], P(('seq', 'head'))
The draws below stay inside these ranges and needn't reach their ends.
Inputs may be any that keep to these rules, and one draw needn't show every extreme that they name: `doc_lengths`: the documents lie in order in the pack and their lengths sum to 32768; document 0 starts at position 0 and every other document d starts strictly inside positions d * 256 to (d + 1) * 256 - 1, excluding the first of these; one length is exactly 510.
All inputs are finite; a program needn't handle non-finite values.
Results may differ from the reference program's by a relative error of at most 0.0062.
Values may be sent and summed in bfloat16 or wider, within the bound.
A program may use at most 64 MiB of HBM per device.

```python
import math
import jax
import jax.numpy as jnp
from jax import lax

KV_RANK = 512
NOPE = 128
ROPE = 64
VDIM = 128
HEADS = 64
TOK_DEV = 128
TOKENS = 32768
DOCS = 128
N_HEAD = 8


def draw_queries(key, part):
    shape = (TOKENS, HEADS, NOPE + ROPE)
    own_key = jax.random.fold_in(key, 11)
    drawn = jnp.clip(2.0 * jax.random.normal(own_key, shape, jnp.float32), -8.0, 8.0)
    return drawn.reshape(TOKENS, HEADS * (NOPE + ROPE)).astype(jnp.bfloat16)


def draw_rope_keys(key, part):
    shape = (TOKENS, ROPE)
    own_key = jax.random.fold_in(key, 12)
    drawn = jnp.clip(jax.random.normal(own_key, shape, jnp.float32), -8.0, 8.0)
    return drawn.astype(jnp.bfloat16)


def draw_doc_lengths(key, part):
    slot_rows = TOKENS // DOCS
    jitter = jax.random.randint(jax.random.fold_in(key, 21), (DOCS,), 1, slot_rows)
    chosen = jax.random.randint(jax.random.fold_in(key, 22), (), 1, DOCS - 1)
    index = jnp.arange(DOCS, dtype=jnp.int32)
    jitter = jnp.where(index == 1, jnp.minimum(jitter, slot_rows - 2), jitter)
    jitter = jnp.where(index == chosen, 1, jitter)
    jitter = jnp.where(index == chosen + 1, slot_rows - 1, jitter)
    jitter = jnp.where(index == 0, 0, jitter)
    starts = index * slot_rows + jitter
    ends = jnp.concatenate([starts[1:], jnp.full((1,), TOKENS, jnp.int32)])
    return (ends - starts).astype(jnp.int32)


def steps_of(key, dims, cuts, low, high):
    factor_of, own = 1.0, jax.random.fold_in(key, 6)
    for position, shards_of in cuts:
        heights = jnp.exp(jax.random.uniform(jax.random.fold_in(own, position), (shards_of,), jnp.float32, low / len(cuts), high / len(cuts)))
        factor_of = factor_of * jnp.repeat(heights, dims[position] // shards_of).reshape([-1 if axis == position else 1 for axis in range(len(dims))])
    return factor_of


def scatter_about(stream_key, extent, spread, bound, pieces=(), held_as=jnp.bfloat16):
    array = spread * jax.random.normal(stream_key, extent, jnp.float32)
    if pieces:
        array = array * steps_of(stream_key, extent, pieces, -0.22, 0.18)
    return jnp.clip(array, -bound, bound).astype(held_as)


def setup_inputs(seed: int = 0) -> dict:
    key_of = jax.random.split(jax.random.key(seed), 7)
    queries = draw_queries(jax.random.fold_in(key_of[6], 71), 0)
    latent = scatter_about(key_of[1], (TOKENS, KV_RANK), 1.0, 6.0, ((0, 256),))
    rope_keys = draw_rope_keys(jax.random.fold_in(key_of[6], 71), 0)
    key_weight = scatter_about(key_of[3], (KV_RANK, HEADS * NOPE), KV_RANK ** -0.5, 0.25, ((0, 32), (1, 8)))
    value_weight = scatter_about(key_of[4], (KV_RANK, HEADS * VDIM), KV_RANK ** -0.5, 0.25, ((0, 32), (1, 8)))
    doc_lengths = draw_doc_lengths(jax.random.fold_in(key_of[6], 71), 0)
    return dict(queries=queries, latent=latent, rope_keys=rope_keys, key_weight=key_weight, value_weight=value_weight, doc_lengths=doc_lengths)


def reference(queries, latent, rope_keys, key_weight, value_weight, doc_lengths):
    total_rows = queries.shape[0]
    group_rows = TOK_DEV * N_HEAD
    block_rows = min(512, group_rows)
    qk_width = NOPE + ROPE
    key_span = group_rows + block_rows
    score_scale = 1.0 / math.sqrt(qk_width)
    starts = (jnp.cumsum(doc_lengths) - doc_lengths).astype(jnp.int32)
    places = jnp.arange(total_rows, dtype=jnp.int32)
    started = (starts[None, :] <= places[:, None]).astype(jnp.int32)
    doc_of = (lax.optimization_barrier(jnp.sum(started, axis=1)) - 1).astype(jnp.int32)
    keys = jnp.dot(latent, key_weight, preferred_element_type=jnp.float32).astype(jnp.bfloat16)
    values = jnp.dot(latent, value_weight, preferred_element_type=jnp.float32).astype(jnp.bfloat16)
    keys_front = jnp.concatenate([jnp.zeros((group_rows, keys.shape[1]), jnp.bfloat16), keys], axis=0)
    values_front = jnp.concatenate([jnp.zeros((group_rows, values.shape[1]), jnp.bfloat16), values], axis=0)
    rope_front = jnp.concatenate([jnp.zeros((group_rows, ROPE), jnp.bfloat16), rope_keys], axis=0)
    docs_front = jnp.concatenate([-jnp.ones((group_rows,), jnp.int32), doc_of], axis=0)

    def one_block(q_index):
        q_start = (q_index * block_rows).astype(jnp.int32)
        q_block = lax.dynamic_slice_in_dim(queries, q_start, block_rows, 0).astype(jnp.float32)
        q_block = q_block.reshape(block_rows, HEADS, qk_width)
        k_nope = lax.dynamic_slice_in_dim(keys_front, q_start, key_span, 0).astype(jnp.float32)
        k_nope = k_nope.reshape(key_span, HEADS, NOPE)
        k_rope = lax.dynamic_slice_in_dim(rope_front, q_start, key_span, 0).astype(jnp.float32)
        k_values = lax.dynamic_slice_in_dim(values_front, q_start, key_span, 0).astype(jnp.float32)
        k_values = k_values.reshape(key_span, HEADS, VDIM)
        q_docs = lax.dynamic_slice_in_dim(doc_of, q_start, block_rows, 0)
        k_docs = lax.dynamic_slice_in_dim(docs_front, q_start, key_span, 0)
        q_places = q_start + jnp.arange(block_rows, dtype=jnp.int32)
        k_places = q_start - group_rows + jnp.arange(key_span, dtype=jnp.int32)
        scores = jnp.einsum('ihd,jhd->hij', q_block[:, :, :NOPE], k_nope)
        scores = (scores + jnp.einsum('ihd,jd->hij', q_block[:, :, NOPE:], k_rope)) * score_scale
        allowed = (q_docs[:, None] == k_docs[None, :]) & (k_places[None, :] <= q_places[:, None])
        scores = jnp.where(allowed[None, :, :], scores, -jnp.inf)
        row_peak = lax.optimization_barrier(jnp.max(scores, axis=2, keepdims=True))
        expo = jnp.exp(scores - row_peak)
        row_sum = lax.optimization_barrier(jnp.sum(expo, axis=2))
        rounded = lax.optimization_barrier(expo.astype(jnp.bfloat16)).astype(jnp.float32)
        mixed = jnp.einsum('hij,jhd->ihd', rounded, k_values) / jnp.transpose(row_sum)[:, :, None]
        return mixed.reshape(block_rows, HEADS * VDIM).astype(jnp.bfloat16)
    attended = lax.map(one_block, jnp.arange(total_rows // block_rows, dtype=jnp.int32))
    return attended.reshape(total_rows, HEADS * VDIM)
```

```python
import functools
import math

import jax
import jax.numpy as jnp
from jax import lax
from jax.experimental import pallas as pl
from jax.experimental.pallas import tpu as pltpu
from jax.sharding import Mesh
from jax.sharding import PartitionSpec as P

NOPE = 128
ROPE = 64
VDIM = 128
PAIR = 384
NX, NY, NZ, NC = 4, 4, 8, 2
HEADS_EACH = 8
SLAB = 16
TOK = 128
KEYS = 6 * TOK
WIN = 5 * TOK
LATENT = 512
LOWEST = -1e30
EXP_SCALE = math.log2(math.e) / math.sqrt(NOPE + ROPE)
SIZES = {"x": NX, "y": NY, "z": NZ}

X_LAST = (0, 1, 2)
Y_LAST = (3, 4, 5)
Z_LAST = (6, 7)
FULL = {"x": (0, NX), "y": (0, NY), "z": (0, NZ)}


class Transfer:
    def __init__(self, name, kind, where, target, deps, link, size, hops=1):
        self.name, self.kind, self.where, self.target = name, kind, where, target
        self.deps, self.link, self.size, self.hops = list(deps), link, size, hops


def weight_transfers():
    out = []

    def own(**over):
        spot = {"x": ("at", 0), "y": ("at", 0), "z": ("at", 0)}
        spot.update(over)
        return spot

    def size_of(spot, heads):
        count = 1
        for axis in "xyz":
            what = spot[axis]
            count *= 1 if what[0] == "at" else what[1]
        return count * heads[1] * SLAB * 2 * NOPE * 2

    def add(name, spot, heads, target, deps, hops=1):
        axis, step = target
        link = axis + ("+" if step > 0 else "-")
        out.append(Transfer(name, "w", (spot, heads), target, deps, link, size_of(spot, heads), hops))
        return name

    def direct(tag, axis, heads, deps):
        got = []
        n = SIZES[axis]
        for step in [s for d in range(1, n // 2 + 1) for s in ((d, -d) if 2 * d < n else (d,))]:
            got.append(add(f"{tag}.{axis}{step}", own(), heads, (axis, step), deps, abs(step)))
        return got

    def ring(tag, axis, spot, heads, deps, half_axis):
        n = SIZES[axis]
        got = {0: list(deps)}
        lo = spot[half_axis][1] // 2
        for sign in (1, -1):
            last = list(deps)
            for k in range(1, n // 2 + 1):
                piece = dict(spot)
                piece[axis] = ("at", -sign * (k - 1))
                if k == n // 2:
                    piece[half_axis] = (0 if sign > 0 else lo, lo)
                name = add(f"{tag}.{axis}{'+' if sign > 0 else '-'}{k}", piece, heads, (axis, sign), last)
                last = [name]
                if k == n // 2:
                    got.setdefault(n // 2, []).append(name)
                else:
                    got[-sign * k] = [name]
        return got

    local = ["load"]
    ready = {}
    first = {}
    for i in range(3):
        for h in (X_LAST[i], Y_LAST[i]):
            first[h] = direct(f"f{h}", "z", (h, 1), local)
        if i == 0:
            zl = (Z_LAST[0], len(Z_LAST))
            c1 = direct("cx", "x", zl, local)
            c2 = ring("cy", "y", own(x=FULL["x"]), zl, c1 + local, "x")
            c_all = sum(c2.values(), [])
    for i in range(3):
        h = X_LAST[i]
        got = ring(f"a{h}", "y", own(z=FULL["z"]), (h, 1), first[h] + local, "z")
        all_y = sorted(set(sum(got.values(), [])))
        got = ring(f"a{h}", "x", own(z=FULL["z"], y=FULL["y"]), (h, 1), all_y, "z")
        for dx, names in got.items():
            ready[("a", h, dx)] = sorted(set(names))
        h = Y_LAST[i]
        got = ring(f"b{h}", "x", own(z=FULL["z"]), (h, 1), first[h] + local, "z")
        all_x = sorted(set(sum(got.values(), [])))
        got = ring(f"b{h}", "y", own(z=FULL["z"], x=FULL["x"]), (h, 1), all_x, "z")
        ready[("b", h, None)] = sorted(set(sum(got.values(), [])))
        if i < 2:
            h = Z_LAST[i]
            got = ring(f"c{h}", "z", own(x=FULL["x"], y=FULL["y"]), (h, 1), sorted(set(c_all)), "x")
            ready[("c", h, None)] = sorted(set(sum(got.values(), [])))
    return out, ready


def other_transfers():
    lat = TOK * (LATENT + 128) * 2
    q = TOK * 4 * PAIR * 2
    out = [
        Transfer("lat.next", "lat", ("in", 2), "next", [], "x+", lat),
        Transfer("lat.core", "lat", ("in", 4), "core", [], "c", lat),
        Transfer("lat.next2", "lat", (2, 0), "next", ["lat.next"], "x+", lat),
        Transfer("lat.core1", "lat", (2, 2), "core", ["lat.next"], "c", lat),
        Transfer("lat.core2", "lat", (0, 0), "core", ["lat.next2"], "c", lat),
    ]
    for x in range(NX):
        out.append(Transfer(f"q{x}", "q", x, "core", [], "c", q))
    lat_names = [t.name for t in out if t.kind == "lat"]
    return out, lat_names


def plan(transfers, units, head_us, rate=46.6e3, d2d=300e3):
    by_name = {t.name: t for t in transfers}
    free, arrive, sent = {}, {}, set()
    order, seen = [], set()
    now = 0.0

    def issue():
        for t in transfers:
            if t.name not in sent and all(d in seen for d in t.deps):
                begin = max(now, free.get(t.link, 0.0))
                free[t.link] = begin + t.size * t.hops / (d2d if t.link == "c" else rate)
                arrive[t.name] = free[t.link] + 1.0 + 0.75 * t.hops
                sent.add(t.name)
                order.append(("send", t.name))

    order.append(("load", None))
    seen.add("load")
    issue()
    todo = list(units)
    while todo or len(seen) <= len(transfers):
        waiting = sorted((when, name) for name, when in arrive.items() if name not in seen)
        unit = next((u for u in todo if all(d in seen for d in u[1])), None)
        if waiting and (waiting[0][0] <= now or unit is None):
            when, name = waiting[0]
            now = max(now, when)
            seen.add(name)
            order.append(("wait", name))
            issue()
        else:
            todo.remove(unit)
            order.append(("head", unit[0]))
            now += head_us * unit[2]
    order.append(("end", now))
    return order


def head_units(ready, after):
    units = []
    for (kind, h, dx), names in ready.items():
        units.append(((kind, h, dx), names + after, 1 if kind == "a" else NX))
    return units


def kernel(order, index, parts, q_ref, lat_ref, rope_ref, kw_ref, vw_ref, len_ref, out_ref,
           wbuf, qb, latb, ropeb, rope2, kext0, kext1, vbuf, bias, outb,
           send_sem, recv_sem, load_sem, out_sem, give_sem, take_sem):
    me = {a: lax.axis_index(a) for a in "xyz"}
    core = lax.axis_index("c")
    other = 1 - core
    chip = (me["z"] * NY + me["y"]) * NX + me["x"]

    def at(axis, step):
        return lax.rem(me[axis] + step + 2 * SIZES[axis], SIZES[axis])

    def chip_id(step):
        b = lax.rem(chip + step + NX * NY * NZ, NX * NY * NZ)
        return {"z": b // (NY * NX), "y": lax.rem(b // NX, NY), "x": lax.rem(b, NX)}

    def device(target):
        if target == "core":
            return {"c": other}
        if target == "next":
            return chip_id(1)
        axis, step = target
        return {axis: at(axis, step)}

    barrier = pltpu.get_barrier_semaphore()
    greeted = [{"c": other}, chip_id(1), chip_id(-1)]
    greeted += [{"x": at("x", s)} for s in range(1, NX)]
    greeted += [{"y": at("y", s)} for s in range(1, NY)]
    greeted += [{"z": at("z", s)} for s in range(1, NZ)]
    for d in greeted:
        pl.semaphore_signal(barrier, inc=1, device_id=d, device_id_type=pl.DeviceIdType.MESH)

    loads = []

    def load(src, dst):
        c = pltpu.make_async_copy(src, dst, load_sem.at[len(loads)])
        c.start()
        loads.append(c)

    for h in range(HEADS_EACH):
        for part, ref in enumerate((kw_ref, vw_ref)):
            load(ref.at[:, pl.ds(h * NOPE, NOPE)],
                 wbuf.at[me["x"], h, me["z"], me["y"], :, pl.ds(part * NOPE, NOPE)])
    early = len(loads)
    load(lat_ref, latb.at[4 + core])
    load(rope_ref, ropeb.at[4 + core])
    for x in range(NX):
        start = pl.multiple_of((2 * x + core) * 4 * PAIR, 128)
        load(q_ref.at[:, pl.ds(start, 4 * PAIR)], qb.at[core, x])

    def weight_spot(where):
        spot, heads = where
        idx = {}
        for axis in "xyz":
            what = spot[axis]
            idx[axis] = at(axis, what[1]) if what[0] == "at" else pl.ds(what[0], what[1])
        return wbuf.at[idx["x"], pl.ds(heads[0], heads[1]), idx["z"], idx["y"]]

    def copies(name):
        t = parts[name]
        k = index[name]
        if t.kind == "w":
            pairs = [(weight_spot(t.where), weight_spot(t.where))]
        elif t.kind == "lat":
            src, dst = t.where
            if src == "in":
                pairs = [(lat_ref, latb.at[dst + core]), (rope_ref, ropeb.at[dst + core])]
            else:
                pairs = [(latb.at[src + core], latb.at[dst + core]),
                         (ropeb.at[src + core], ropeb.at[dst + core])]
        else:
            start = pl.multiple_of((2 * t.where + other) * 4 * PAIR, 128)
            pairs = [(q_ref.at[:, pl.ds(start, 4 * PAIR)], qb.at[core, t.where])]
        return [
            pltpu.make_async_remote_copy(
                src_ref=s, dst_ref=d, send_sem=send_sem.at[k + i], recv_sem=recv_sem.at[k + i],
                device_id=device(t.target), device_id_type=pl.DeviceIdType.MESH,
            )
            for i, (s, d) in enumerate(pairs)
        ]

    lens = len_ref[...].astype(jnp.float32)
    rows = lax.broadcasted_iota(jnp.int32, (128, 128), 0)
    cols = lax.broadcasted_iota(jnp.int32, (128, 128), 1)
    as_rows = jnp.broadcast_to(lens, (128, 128))
    as_column = jnp.sum(jnp.where(rows == cols, as_rows, 0.0), axis=1, keepdims=True)
    starts = jnp.sum(jnp.where(rows < cols, as_column, 0.0), axis=0, keepdims=True)
    for half in range(2):
        base = chip * (NC * TOK) + half * TOK
        q_pos = (base + lax.broadcasted_iota(jnp.int32, (TOK, 128), 0)).astype(jnp.float32)
        started = jnp.where(starts <= q_pos, starts, 0.0)
        q_start = jnp.max(started, axis=1, keepdims=True)
        k_pos = (base - 4 * TOK + lax.broadcasted_iota(jnp.int32, (TOK, WIN), 1)).astype(jnp.float32)
        q_row = (base + lax.broadcasted_iota(jnp.int32, (TOK, WIN), 0)).astype(jnp.float32)
        seen = (k_pos >= q_start) & (k_pos <= q_row)
        bias[half] = jnp.where(seen, 0.0, LOWEST)

    lane = lax.broadcasted_iota(jnp.int32, (KEYS, 128), 1)

    def prepare():
        r = ropeb[...].reshape(KEYS, ROPE).astype(jnp.float32)
        r = jnp.concatenate([r, r], axis=1)
        rope2[...] = r.astype(jnp.bfloat16)
        kext0[:, NOPE:] = jnp.where(lane < ROPE, r, 0.0).astype(jnp.bfloat16)

    def one_head(x, h):
        w = wbuf[x, h].reshape(LATENT, 2 * NOPE)
        kv = jnp.dot(latb[...].reshape(KEYS, LATENT), w, preferred_element_type=jnp.float32)
        keys = kv[:, :NOPE]
        vbuf[...] = kv[:, NOPE:].astype(jnp.bfloat16)
        if h % 2 == 0:
            kext = kext0
            kext0[:, :NOPE] = keys.astype(jnp.bfloat16)
        else:
            kext = kext1
            turned = pltpu.roll(keys, 64, 1)
            kext1[:, :NOPE] = jnp.where(lane < 64, 0.0, turned).astype(jnp.bfloat16)
            kext1[:, NOPE:] = jnp.where(lane < 64, turned.astype(jnp.bfloat16), rope2[...])
        column = (h // 2) * PAIR + (h % 2) * 128
        for half in range(2):
            q = qb[half, x, :, pl.ds(column, 256)]
            s = lax.dot_general(q, kext[pl.ds(half * TOK, WIN), :], (((1,), (1,)), ((), ())),
                                preferred_element_type=jnp.float32)
            s = s + bias[half]
            peak = jnp.max(s, axis=1, keepdims=True)
            expo = jnp.exp2((s - peak) * EXP_SCALE)
            total = jnp.sum(expo, axis=1, keepdims=True)
            mixed = jnp.dot(expo.astype(jnp.bfloat16), vbuf[pl.ds(half * TOK, WIN), :],
                            preferred_element_type=jnp.float32)
            outb[half, x, h] = (mixed / total).astype(jnp.bfloat16)

    def out_copies(x, h):
        mine = pl.multiple_of(((2 * x + core) * HEADS_EACH + h) * VDIM, VDIM)
        slot = x * HEADS_EACH + h
        spot = out_ref.at[:, pl.ds(mine, VDIM)]
        local = pltpu.make_async_copy(outb.at[core, x, h], spot, out_sem.at[slot])
        away = pltpu.make_async_remote_copy(
            src_ref=outb.at[other, x, h], dst_ref=spot,
            send_sem=give_sem.at[slot], recv_sem=take_sem.at[slot],
            device_id={"c": other}, device_id_type=pl.DeviceIdType.MESH,
        )
        return local, away

    def put_out(done):
        for x, h in done:
            for c in out_copies(x, h):
                c.start()

    pl.semaphore_wait(barrier, len(greeted))
    sent, finished, prepared, loaded = [], [], False, False
    for what, name in order:
        if what == "load":
            for c in loads[:early]:
                c.wait()
        elif what == "send":
            for c in copies(name):
                c.start()
            sent.append(name)
        elif what == "wait":
            for c in copies(name):
                c.wait_recv()
        elif what == "head":
            if not prepared:
                for c in loads[early:]:
                    c.wait()
                prepare()
                prepared = True
            kind, h, dx = name
            if kind == "a":
                x = at("x", dx)
                one_head(x, h)
                done = [(x, h)]
            else:
                lax.fori_loop(0, NX, lambda x, _: (one_head(x, h), 0)[1], 0)
                done = [(x, h) for x in range(NX)]
            put_out(finished)
            finished = done
            all_done = None
    put_out(finished)
    for name in sent:
        for c in copies(name):
            c.wait_send()
    for x in range(NX):
        for h in range(HEADS_EACH):
            local, away = out_copies(x, h)
            local.wait()
            away.wait()


def shards(queries, latent, rope_keys, key_weight, value_weight, doc_lengths):
    weights, ready = weight_transfers()
    rest, lat_names = other_transfers()
    lats = [t for t in rest if t.kind == "lat"]
    qs = [t for t in rest if t.kind == "q"]
    transfers = lats[:2] + weights + lats[2:] + qs
    after = lat_names + [t.name for t in qs] + ["load"]
    order = plan(transfers, head_units(ready, after), HEAD_US)[:-1]
    index, at = {}, 0
    for t in transfers:
        index[t.name] = at
        at += 2 if t.kind == "lat" else 1
    parts = {t.name: t for t in transfers}
    hbm = pl.BlockSpec(memory_space=pl.ANY)
    bf = jnp.bfloat16
    return pl.pallas_call(
        functools.partial(kernel, order, index, parts),
        out_shape=jax.ShapeDtypeStruct((TOK, 64 * VDIM), bf),
        in_specs=[hbm] * 5 + [pl.BlockSpec(memory_space=pltpu.VMEM)],
        out_specs=hbm,
        scratch_shapes=[
            pltpu.VMEM((NX, HEADS_EACH, NZ, NY, SLAB, 2 * NOPE), bf),
            pltpu.VMEM((NC, NX, TOK, 4 * PAIR), bf),
            pltpu.VMEM((6, TOK, LATENT), bf),
            pltpu.VMEM((6, TOK, ROPE), bf),
            pltpu.VMEM((KEYS, 128), bf),
            pltpu.VMEM((KEYS, 256), bf),
            pltpu.VMEM((KEYS, 256), bf),
            pltpu.VMEM((KEYS, VDIM), bf),
            pltpu.VMEM((NC, TOK, WIN), jnp.float32),
            pltpu.VMEM((NC, NX, HEADS_EACH, TOK, VDIM), bf),
            pltpu.SemaphoreType.DMA((at,)),
            pltpu.SemaphoreType.DMA((at,)),
            pltpu.SemaphoreType.DMA((2 * HEADS_EACH + 2 + NX,)),
            pltpu.SemaphoreType.DMA((NX * HEADS_EACH,)),
            pltpu.SemaphoreType.DMA((NX * HEADS_EACH,)),
            pltpu.SemaphoreType.DMA((NX * HEADS_EACH,)),
        ],
        compiler_params=pltpu.CompilerParams(
            collective_id=0, has_side_effects=True, vmem_limit_bytes=56 * 2**20
        ),
    )(queries, latent, rope_keys, key_weight, value_weight, doc_lengths.reshape(1, -1))


HEAD_US = 0.75


def solution(mesh):
    torus = Mesh(mesh.devices.reshape(NZ, NY, NX, NC), ("z", "y", "x", "c"))
    rows = P(("z", "y", "x", "c"), None)
    weight = P(("z", "y"), ("x", "c"))
    return jax.shard_map(
        shards, mesh=torus, in_specs=(rows, rows, rows, weight, weight, P()), out_specs=rows,
        check_vma=False,
    )
```

```python
import functools
import math

import jax
import jax.numpy as jnp
from jax import lax
from jax.experimental import pallas as pl
from jax.experimental.pallas import tpu as pltpu
from jax.sharding import Mesh
from jax.sharding import PartitionSpec as P

NOPE = 128
ROPE = 64
VDIM = 128
PAIR = 384
NX, NY, NZ, NC = 4, 4, 8, 2
HEADS_EACH = 8
SLAB = 16
TOK = 128
KEYS = 6 * TOK
WIN = 5 * TOK
LATENT = 512
LOWEST = -1e30
EXP_SCALE = math.log2(math.e) / math.sqrt(NOPE + ROPE)
SIZES = {"x": NX, "y": NY, "z": NZ}
FULL = {"x": (0, NX), "y": (0, NY), "z": (0, NZ)}

X_LAST = (0, 1, 2)
Y_LAST = (5, 4, 3)
Z_LAST = (6, 7)
LATER = (1, 4)
FINE = (True, False, False)
X_FORWARD = 3
DEPTH = 4.0
UNIT_US = {1: 1.1, 2: 1.5, 4: 3.0}
NT = (((1,), (1,)), ((), ()))
TN = (((0,), (0,)), ((), ()))


def PRIORITY(t, reach):
    return 0


class Transfer:
    def __init__(self, name, kind, where, target, deps, link, size, hops=1):
        self.name, self.kind, self.where, self.target = name, kind, where, target
        self.deps, self.link, self.size, self.hops = list(deps), link, size, hops


def weight_transfers():
    out, ready = [], {}

    def own(**over):
        spot = {"x": ("at", 0), "y": ("at", 0), "z": ("at", 0)}
        spot.update(over)
        return spot

    def add(name, spot, heads, target, deps, hops=1):
        axis, step = target
        count = heads[1]
        for a in "xyz":
            count *= 1 if spot[a][0] == "at" else spot[a][1]
        link = axis + ("+" if step > 0 else "-")
        size = count * SLAB * 2 * NOPE * 2
        out.append(Transfer(name, "w", (spot, heads), target, deps, link, size, hops))
        return name

    def direct(tag, axis, heads, deps, far=1):
        n = SIZES[axis]
        steps = [s for d in range(1, n // 2) for s in (d, -d)] + [far * (n // 2)]
        return [add(f"{tag}{axis}{s}", own(), heads, (axis, s), deps, abs(s)) for s in steps]

    def ring(tag, axis, spot, heads, deps, half_axis, forward=None):
        n = SIZES[axis]
        got = {0: list(deps)}
        lo, width = heads if half_axis == "h" else spot[half_axis]
        cut = width // 2 if forward is None else forward
        for sign in (1, -1):
            last = list(deps)
            for k in range(1, n // 2 + 1):
                piece, part = dict(spot), heads
                piece[axis] = ("at", -sign * (k - 1))
                if k == n // 2:
                    share = (lo, cut) if sign > 0 else (lo + cut, width - cut)
                    if share[1] == 0:
                        continue
                    if half_axis == "h":
                        part = share
                    else:
                        piece[half_axis] = share
                name = add(f"{tag}{axis}{'+' if sign > 0 else '-'}{k}", piece, part, (axis, sign), last)
                last = [name]
                got.setdefault(n // 2 if k == n // 2 else -sign * k, []).append(name)
        return got

    def last_ring(tag, axis, inner, spot, heads, units, forward=None):
        got = {}
        for offset, deps in units.items():
            piece = dict(spot)
            if offset is None:
                piece[inner] = FULL[inner]
            else:
                piece[inner] = ("at", offset)
            for o, names in ring(f"{tag}u{offset}", axis, piece, heads, deps, "z", forward).items():
                got.setdefault(o, []).extend(names)
        return {o: sorted(set(names)) for o, names in got.items()}

    def whole(units):
        return {None: sorted(set(sum(units.values(), [])))}

    local = ["load"]
    first = {X_LAST[0]: direct("f0", "z", (X_LAST[0], 1), local, 1),
             Y_LAST[0]: direct("f1", "z", (Y_LAST[0], 1), local, -1)}
    zl = (Z_LAST[0], len(Z_LAST))
    c_first = direct("fc", "x", zl, local, -1)
    later = ring("f2", "z", own(), LATER, local, "h")
    later = sorted(set(sum(later.values(), [])))
    for h in X_LAST[1:] + Y_LAST[1:]:
        first[h] = later
    c_units = ring("c", "y", own(x=FULL["x"]), zl, c_first + local, "x")
    c_all = whole(c_units)[None]
    for i in range(3):
        h = X_LAST[i]
        units = ring(f"a{i}", "y", own(z=FULL["z"]), (h, 1), first[h] + local, "z")
        if not FINE[i]:
            units = whole(units)
        got = last_ring(f"a{i}", "x", "y", own(z=FULL["z"]), (h, 1), units, X_FORWARD)
        ready[("a", h, (0,))] = got[0]
        ready[("a", h, (-1, 1))] = sorted(set(got[-1] + got[1]))
        ready[("a", h, (2,))] = got[2]
        h = Y_LAST[i]
        units = ring(f"b{i}", "x", own(z=FULL["z"]), (h, 1), first[h] + local, "z")
        if not FINE[i]:
            units = whole(units)
        got = last_ring(f"b{i}", "y", "x", own(z=FULL["z"]), (h, 1), units)
        ready[("b", h, None)] = sorted(set(sum(got.values(), [])))
        if i < 2:
            h = Z_LAST[i]
            got = ring(f"c{i}", "z", own(x=FULL["x"], y=FULL["y"]), (h, 1), c_all, "x")
            ready[("c", h, None)] = sorted(set(sum(got.values(), [])))
    return out, ready


def other_transfers():
    lat = TOK * (LATENT + 64) * 2
    q = TOK * 4 * PAIR * 2
    out = [
        Transfer("lat.next", "lat", ("in", 2), "next", [], "x+", lat),
        Transfer("lat.core", "lat", ("in", 4), "core", [], "c", lat),
        Transfer("lat.next2", "lat", (2, 0), "next", ["lat.next"], "x+", lat),
        Transfer("lat.core1", "lat", (2, 2), "core", ["lat.next"], "c", lat),
        Transfer("lat.core2", "lat", (0, 0), "core", ["lat.next2"], "c", lat),
    ]
    lat_names = [t.name for t in out]
    for x in range(NX):
        out.append(Transfer(f"q{x}", "q", x, "core", [], "c", q))
    return out, lat_names


def plan(transfers, units, rate=46.6e3, d2d=600e3, depth=4.0):
    by_name = {t.name: t for t in transfers}
    tail = {}
    follow = {}
    for t in transfers:
        for d in t.deps:
            follow.setdefault(d, []).append(t.name)

    def cost(t):
        return t.size * t.hops / (d2d if t.link == "c" else rate)

    def reach(name):
        if name not in tail:
            tail[name] = cost(by_name[name]) + 1.0 + 0.75 * by_name[name].hops + max(
                [reach(f) for f in follow.get(name, [])], default=0.0)
        return tail[name]

    rank = {t.name: (PRIORITY(t, reach(t.name)), i) for i, t in enumerate(transfers)}
    free, arrive, sent = {}, {}, set()
    order, seen = [], set()
    now = 0.0

    def issue():
        for t in sorted(transfers, key=lambda t: rank[t.name]):
            if t.name not in sent and all(d in seen for d in t.deps):
                if free.get(t.link, 0.0) - now > depth:
                    continue
                free[t.link] = max(now, free.get(t.link, 0.0)) + cost(t)
                arrive[t.name] = free[t.link] + 1.0 + 0.75 * t.hops
                sent.add(t.name)
                order.append(("send", t.name))

    order.append(("load", None))
    seen.add("load")
    issue()
    todo = list(units)
    busy = 0.0
    while todo or len(seen) <= len(transfers):
        waiting = sorted((when, name) for name, when in arrive.items() if name not in seen)
        unit = next((u for u in todo if all(d in seen for d in u[1])), None)
        if waiting and (waiting[0][0] <= now or unit is None):
            when, name = waiting[0]
            now = max(now, when)
            seen.add(name)
            order.append(("wait", name))
            issue()
        elif unit is not None:
            todo.remove(unit)
            order.append(("head", unit[0]))
            now += unit[2]
            busy += unit[2]
            issue()
        else:
            now += 0.2
            issue()
    return order, now, max(arrive.values(), default=0), busy


def kernel(order, index, parts, q_ref, lat_ref, rope_ref, kw_ref, vw_ref, len_ref, out_ref,
           wbuf, qb, latb, ropeb, rope2, kexts, vbufs, bias, outb,
           send_sem, recv_sem, load_sem, out_sem, give_sem, take_sem):
    me = {a: lax.axis_index(a) for a in "xyz"}
    core = lax.axis_index("c")
    other = 1 - core
    chip = (me["z"] * NY + me["y"]) * NX + me["x"]

    def at(axis, step):
        return lax.rem(me[axis] + step + 2 * SIZES[axis], SIZES[axis])

    def chip_id(step):
        b = lax.rem(chip + step + NX * NY * NZ, NX * NY * NZ)
        return {"z": b // (NY * NX), "y": lax.rem(b // NX, NY), "x": lax.rem(b, NX)}

    def device(target):
        if target == "core":
            return {"c": other}
        if target == "next":
            return chip_id(1)
        axis, step = target
        return {axis: at(axis, step)}

    barrier = pltpu.get_barrier_semaphore()
    greeted = [{"c": other}, chip_id(1), chip_id(-1)]
    greeted += [{a: at(a, s)} for a in "xyz" for s in range(1, SIZES[a])]
    for d in greeted:
        pl.semaphore_signal(barrier, inc=1, device_id=d, device_id_type=pl.DeviceIdType.MESH)

    loads = []

    def load(src, dst):
        c = pltpu.make_async_copy(src, dst, load_sem.at[len(loads)])
        c.start()
        loads.append(c)

    for h in range(HEADS_EACH):
        for part, ref in enumerate((kw_ref, vw_ref)):
            load(ref.at[:, pl.ds(h * NOPE, NOPE)],
                 wbuf.at[me["x"], h, me["z"], me["y"], :, pl.ds(part * NOPE, NOPE)])
    early = len(loads)
    load(lat_ref, latb.at[4 + core])
    load(rope_ref, ropeb.at[4 + core])
    for x in range(NX):
        start = pl.multiple_of((2 * x + core) * 4 * PAIR, 128)
        load(q_ref.at[:, pl.ds(start, 4 * PAIR)], qb.at[x, core])

    def weight_spot(where):
        spot, heads = where
        idx = {}
        for axis in "xyz":
            what = spot[axis]
            idx[axis] = at(axis, what[1]) if what[0] == "at" else pl.ds(what[0], what[1])
        return wbuf.at[idx["x"], pl.ds(heads[0], heads[1]), idx["z"], idx["y"]]

    def copies(name):
        t = parts[name]
        k = index[name]
        if t.kind == "w":
            pairs = [(weight_spot(t.where), weight_spot(t.where))]
        elif t.kind == "lat":
            src, dst = t.where
            if src == "in":
                pairs = [(lat_ref, latb.at[dst + core]), (rope_ref, ropeb.at[dst + core])]
            else:
                pairs = [(latb.at[src + core], latb.at[dst + core]),
                         (ropeb.at[src + core], ropeb.at[dst + core])]
        else:
            start = pl.multiple_of((2 * t.where + other) * 4 * PAIR, 128)
            pairs = [(q_ref.at[:, pl.ds(start, 4 * PAIR)], qb.at[t.where, core])]
        return [
            pltpu.make_async_remote_copy(
                src_ref=s, dst_ref=d, send_sem=send_sem.at[k + i], recv_sem=recv_sem.at[k + i],
                device_id=device(t.target), device_id_type=pl.DeviceIdType.MESH,
            )
            for i, (s, d) in enumerate(pairs)
        ]

    lane = lax.broadcasted_iota(jnp.int32, (KEYS, 128), 1)

    def make_bias():
        lens = len_ref[...].astype(jnp.float32)
        rows = lax.broadcasted_iota(jnp.int32, (128, 128), 0)
        cols = lax.broadcasted_iota(jnp.int32, (128, 128), 1)
        as_rows = jnp.broadcast_to(lens, (128, 128))
        starts = jnp.sum(jnp.where(cols < rows, as_rows, 0.0), axis=1, keepdims=True)
        for half in range(NC):
            base = chip * (NC * TOK) + half * TOK
            q_pos = (base + cols).astype(jnp.float32)
            started = jnp.where(starts <= q_pos, starts, 0.0)
            q_start = jnp.max(started, axis=0, keepdims=True)
            k_pos = (base - 4 * TOK + lax.broadcasted_iota(jnp.int32, (WIN, TOK), 0)).astype(jnp.float32)
            q_row = (base + lax.broadcasted_iota(jnp.int32, (WIN, TOK), 1)).astype(jnp.float32)
            bias[half] = jnp.where((k_pos >= q_start) & (k_pos <= q_row), 0.0, LOWEST)

    def prepare():
        for s in range(6):
            r = ropeb[s].astype(jnp.float32)
            r = jnp.transpose(jnp.concatenate([r, r], axis=0))
            spot = pl.ds(s * TOK, TOK)
            rope2[spot, :] = r.astype(jnp.bfloat16)
            for slot in range(2):
                kexts[2 * slot, spot, NOPE:] = jnp.where(lane[:TOK] < ROPE, r, 0.0).astype(jnp.bfloat16)

    def project(x, h, slot):
        w = wbuf[x, h].reshape(LATENT, 2 * NOPE)
        kv = jnp.dot(latb[...].reshape(KEYS, LATENT), w, preferred_element_type=jnp.float32)
        keys = kv[:, :NOPE]
        vbufs[slot] = kv[:, NOPE:].astype(jnp.bfloat16)
        if h % 2 == 0:
            kexts[2 * slot, :, :NOPE] = keys.astype(jnp.bfloat16)
        else:
            turned = pltpu.roll(keys, 64, 1)
            kexts[2 * slot + 1, :, :NOPE] = jnp.where(lane < 64, 0.0, turned).astype(jnp.bfloat16)
            kexts[2 * slot + 1, :, NOPE:] = jnp.where(lane < 64, turned.astype(jnp.bfloat16), rope2[...])

    def attend(x, h, slot):
        column = (h // 2) * PAIR + (h % 2) * 128
        q = qb[x, :, :, pl.ds(column, 256)].reshape(NC * TOK, 256)
        scores = lax.dot_general(kexts[2 * slot + h % 2], q, NT, preferred_element_type=jnp.float32)
        for half in range(NC):
            at_keys, at_rows = slice(half * TOK, half * TOK + WIN), slice(half * TOK, half * TOK + TOK)
            s = scores[at_keys, at_rows] + bias[half]
            peak = jnp.max(s, axis=0, keepdims=True)
            expo = jnp.exp2((s - peak) * EXP_SCALE)
            total = jnp.sum(expo, axis=0, keepdims=True)
            mixed = lax.dot_general(expo.astype(jnp.bfloat16), vbufs[slot, at_keys, :], TN,
                                    preferred_element_type=jnp.float32)
            under = jnp.transpose(jnp.broadcast_to(total, (TOK, TOK)))
            outb[half, x, h] = (mixed / under).astype(jnp.bfloat16)

    def heads_of(xs, h):
        for slot, x in enumerate(xs):
            project(x, h, slot)
        for slot, x in enumerate(xs):
            attend(x, h, slot)

    def out_copies(x, h):
        mine = pl.multiple_of(((2 * x + core) * HEADS_EACH + h) * VDIM, VDIM)
        slot = x * HEADS_EACH + h
        spot = out_ref.at[:, pl.ds(mine, VDIM)]
        local = pltpu.make_async_copy(outb.at[core, x, h], spot, out_sem.at[slot])
        away = pltpu.make_async_remote_copy(
            src_ref=outb.at[other, x, h], dst_ref=spot,
            send_sem=give_sem.at[slot], recv_sem=take_sem.at[slot],
            device_id={"c": other}, device_id_type=pl.DeviceIdType.MESH,
        )
        return local, away

    def put_out(done):
        for x, h in done:
            for c in out_copies(x, h):
                c.start()

    pl.semaphore_wait(barrier, len(greeted))
    sent, finished, state = [], [], set()
    for what, name in order:
        if what == "load":
            for c in loads[:early]:
                c.wait()
        elif what == "send":
            for c in copies(name):
                c.start()
            sent.append(name)
        elif what == "wait":
            if "bias" not in state:
                make_bias()
                state.add("bias")
            for c in copies(name):
                c.wait_recv()
        elif what == "head":
            if "prepared" not in state:
                for c in loads[early:]:
                    c.wait()
                prepare()
                state.add("prepared")
            kind, h, steps = name
            if kind == "a":
                xs = [at("x", dx) for dx in steps]
                heads_of(xs, h)
            else:
                xs = list(range(NX))
                lax.fori_loop(0, NX // 2, lambda i, _: (heads_of([2 * i, 2 * i + 1], h), 0)[1], 0)
            put_out(finished)
            finished = [(x, h) for x in xs]
    put_out(finished)
    for name in sent:
        for c in copies(name):
            c.wait_send()
    for x in range(NX):
        for h in range(HEADS_EACH):
            local, away = out_copies(x, h)
            local.wait()
            away.wait()


def shards(queries, latent, rope_keys, key_weight, value_weight, doc_lengths):
    weights, ready = weight_transfers()
    rest, lat_names = other_transfers()
    transfers = rest[:2] + weights + rest[2:]
    after = lat_names + [t.name for t in rest if t.kind == "q"] + ["load"]
    units = [(k, v + after, UNIT_US[NX if k[2] is None else len(k[2])]) for k, v in ready.items()]
    order = plan(transfers, units, depth=DEPTH)[0]
    index, at = {}, 0
    for t in transfers:
        index[t.name] = at
        at += 2 if t.kind == "lat" else 1
    parts = {t.name: t for t in transfers}
    hbm = pl.BlockSpec(memory_space=pl.ANY)
    bf = jnp.bfloat16
    return pl.pallas_call(
        functools.partial(kernel, order, index, parts),
        out_shape=jax.ShapeDtypeStruct((TOK, 64 * VDIM), bf),
        in_specs=[hbm] * 5 + [pl.BlockSpec(memory_space=pltpu.VMEM)],
        out_specs=hbm,
        scratch_shapes=[
            pltpu.VMEM((NX, HEADS_EACH, NZ, NY, SLAB, 2 * NOPE), bf),
            pltpu.VMEM((NX, NC, TOK, 4 * PAIR), bf),
            pltpu.VMEM((6, TOK, LATENT), bf),
            pltpu.VMEM((6, ROPE, TOK), bf),
            pltpu.VMEM((KEYS, 128), bf),
            pltpu.VMEM((4, KEYS, 256), bf),
            pltpu.VMEM((2, KEYS, VDIM), bf),
            pltpu.VMEM((NC, WIN, TOK), jnp.float32),
            pltpu.VMEM((NC, NX, HEADS_EACH, TOK, VDIM), bf),
            pltpu.SemaphoreType.DMA((at,)),
            pltpu.SemaphoreType.DMA((at,)),
            pltpu.SemaphoreType.DMA((2 * HEADS_EACH + 2 + NX,)),
            pltpu.SemaphoreType.DMA((NX * HEADS_EACH,)),
            pltpu.SemaphoreType.DMA((NX * HEADS_EACH,)),
            pltpu.SemaphoreType.DMA((NX * HEADS_EACH,)),
        ],
        compiler_params=pltpu.CompilerParams(
            collective_id=0, has_side_effects=True, vmem_limit_bytes=56 * 2**20
        ),
    )(queries, latent, rope_keys.T, key_weight, value_weight, doc_lengths.reshape(1, -1))


def solution(mesh):
    torus = Mesh(mesh.devices.reshape(NZ, NY, NX, NC), ("z", "y", "x", "c"))
    rows = P(("z", "y", "x", "c"), None)
    weight = P(("z", "y"), ("x", "c"))
    return jax.shard_map(
        shards, mesh=torus, in_specs=(rows, rows, rows, weight, weight, P()), out_specs=rows,
        check_vma=False,
    )
```

```python
import functools
import math

import jax
import jax.numpy as jnp
from jax import lax
from jax.experimental import pallas as pl
from jax.experimental.pallas import tpu as pltpu
from jax.sharding import Mesh
from jax.sharding import PartitionSpec as P

NOPE = 128
ROPE = 64
VDIM = 128
PAIR = 384
NX, NY, NZ, NC = 4, 4, 8, 2
HEADS_EACH = 8
SLAB = 16
TOK = 128
KEYS = 6 * TOK
WIN = 5 * TOK
LATENT = 512
LOWEST = -1e30
EXP_SCALE = math.log2(math.e) / math.sqrt(NOPE + ROPE)
SIZES = {"x": NX, "y": NY, "z": NZ}
FULL = {"x": (0, NX), "y": (0, NY), "z": (0, NZ)}

FIRST = [
    ('b', (4, 1), 'x', 'direct', 1),
    ('a', (0, 1), 'z', 'direct', 1),
    ('B', (5, 1), 'z', 'direct', -1),
    ('c', (6, 2), 'x', 'direct', -1),
    ('l', (1, 3), 'z', 'ring', 1),
]
CHAINS = [
    ('a0', 'a', (0, 1), 'zyx', True, ('z', 'z'), 3),
    ('b0', 'B', (5, 1), 'zxy', True, ('z', 'z'), None),
    ('c', 'c', (6, 1), 'xyz', False, ('x', 'x'), None),
    ('d', 'c', (7, 1), 'xyz', False, ('x', 'x'), None),
    ('a1', 'l', (1, 1), 'zyx', False, ('z', 'z'), 3),
    ('b1', 'b', (4, 1), 'xzy', False, ('x', 'x'), None),
    ('a2', 'l', (2, 1), 'zyx', True, ('z', 'z'), 3),
    ('b2', 'l', (3, 1), 'zxy', False, ('z', 'z'), None),
]
DEPTH = 4
LATE = 0.0
FIXED_US = 1.4
HOP_US = 0.9
UNIT_US = {1: 1.15, 2: 1.55, 4: 2.6}
NT = (((1,), (1,)), ((), ()))
TN = (((0,), (0,)), ((), ()))


ORDER = {"fb": -19.4, "fa": -6.0, "fB": -14.9, "fc": -20.8, "fl": -6.7, "a0": -4.4, "a0h0": -0.6, "b0": -5.2, "b0h5": 17.1, "c": 2.0, "ch6": 0.9, "d": 2.7, "dh7": 15.9, "a1": -11.2, "a1h1": 24.8, "b1": -1.6, "b1h4": 10.0, "a2": -19.8, "a2h2": 3.3, "b2": -14.1, "b2h3": 22.7, "lat": -19.1, "q": 9.6}
REACH_SHARE = 0.6


def stage(name):
    if name[0] == "f":
        return name[:2]
    if name[0] in "lq":
        return "lat" if name[0] == "l" else "q"
    return name[:name.index("u")] if "u" in name else name[:-3]


def PRIORITY(t, reach):
    return ORDER[stage(t.name)] - REACH_SHARE * reach


class Transfer:
    def __init__(self, name, kind, where, target, deps, link, size, hops=1, late=0.0):
        self.name, self.kind, self.where, self.target = name, kind, where, target
        self.deps, self.link, self.size, self.hops, self.late = list(deps), link, size, hops, late


def weight_transfers():
    out, ready = [], {}

    def own(**over):
        spot = {"x": ("at", 0), "y": ("at", 0), "z": ("at", 0)}
        spot.update(over)
        return spot

    def add(name, spot, heads, target, deps, hops=1):
        axis, step = target
        count = heads[1]
        for a in "xyz":
            count *= 1 if spot[a][0] == "at" else spot[a][1]
        link = axis + ("+" if step > 0 else "-")
        size = count * SLAB * 2 * NOPE * 2
        out.append(Transfer(name, "w", (spot, heads), target, deps, link, size, hops))
        return name

    def direct(tag, axis, heads, deps, far=1):
        n = SIZES[axis]
        steps = [s for d in range(1, n // 2) for s in (d, -d)] + [far * (n // 2)]
        return [add(f"{tag}{axis}{s}", own(), heads, (axis, s), deps, abs(s)) for s in steps]

    def ring(tag, axis, spot, heads, deps, half_axis, forward=None):
        n = SIZES[axis]
        got = {0: list(deps)}
        lo, width = heads if half_axis == "h" else spot.get(half_axis, (0, 2))
        cut = width // 2 if forward is None else forward
        for sign in (1, -1):
            last = list(deps)
            for k in range(1, n // 2 + 1):
                piece, part = dict(spot), heads
                piece[axis] = ("at", -sign * (k - 1))
                if k == n // 2:
                    share = (lo, cut) if sign > 0 else (lo + cut, width - cut)
                    if share[1] == 0:
                        continue
                    if half_axis == "h":
                        part = share
                    elif half_axis:
                        piece[half_axis] = share
                name = add(f"{tag}{axis}{'+' if sign > 0 else '-'}{k}", piece, part, (axis, sign), last)
                last = [name]
                got.setdefault(n // 2 if k == n // 2 else -sign * k, []).append(name)
        return got

    def last_ring(tag, axis, inner, spot, heads, units, half_axis, forward=None):
        got = {}
        for offset, deps in units.items():
            piece, way = dict(spot), forward
            if offset is None:
                piece[inner] = FULL[inner]
            else:
                piece[inner] = ("at", offset)
            for o, names in ring(f"{tag}u{offset}", axis, piece, heads, deps, half_axis, way).items():
                got.setdefault(o, []).extend(names)
        return {o: sorted(set(names)) for o, names in got.items()}

    def merged(units):
        return {None: sorted(set(sum(units.values(), [])))}

    local = ["load"]
    first = {}
    for tag, heads, axis, how, far in FIRST:
        if how == "direct":
            names = direct(f"f{tag}", axis, heads, local, far)
        else:
            names = sorted(set(sum(ring(f"f{tag}", axis, own(), heads, local, "h").values(), [])))
        first[tag] = names + local
    for tag, source, heads, axes, fine, halves, forward in CHAINS:
        a, b, c = axes
        units = ring(f"{tag}", b, own(**{a: FULL[a]}), heads, first[source], halves[0])
        if not fine:
            units = merged(units)
        for h in range(heads[0], heads[0] + heads[1]):
            got = last_ring(f"{tag}h{h}", c, b, own(**{a: FULL[a]}), (h, 1), units, halves[1], forward)
            if c == "x":
                ready[("a", h, (0,))] = got[0]
                ready[("a", h, (-1, 1))] = sorted(set(got[-1] + got[1]))
                ready[("a", h, (2,))] = got[2]
            else:
                ready[("b", h, None)] = sorted(set(sum(got.values(), [])))
    return out, ready


def other_transfers():
    lat = TOK * (LATENT + 64) * 2
    q = TOK * 4 * PAIR * 2
    out = [
        Transfer("lat.next", "lat", ("in", 2), "next", [], "x+", lat, 1, LATE),
        Transfer("lat.core", "lat", ("in", 4), "core", [], "c", lat),
        Transfer("lat.next2", "lat", (2, 0), "next", ["lat.next"], "x+", lat, 1, LATE),
        Transfer("lat.core1", "lat", (2, 2), "core", ["lat.next"], "c", lat),
        Transfer("lat.core2", "lat", (0, 0), "core", ["lat.next2"], "c", lat),
    ]
    lat_names = [t.name for t in out]
    for x in range(NX):
        out.append(Transfer(f"q{x}", "q", x, "core", [], "c", q))
    return out, lat_names


def plan(transfers, units, rate=45e3, d2d=500e3, depth=4.0):
    by_name = {t.name: t for t in transfers}
    tail, follow = {}, {}
    for t in transfers:
        for d in t.deps:
            follow.setdefault(d, []).append(t.name)

    def cost(t):
        return t.size * t.hops / (d2d if t.link == "c" else rate)

    def delay(t):
        return FIXED_US + HOP_US * t.hops + t.late

    def reach(name):
        if name not in tail:
            tail[name] = cost(by_name[name]) + delay(by_name[name]) + max(
                [reach(f) for f in follow.get(name, [])], default=0.0)
        return tail[name]

    rank = {t.name: (PRIORITY(t, reach(t.name)), i) for i, t in enumerate(transfers)}
    free, arrive, sent = {}, {}, set()
    order, seen = [], set()
    now = 0.0

    def issue():
        for t in sorted(transfers, key=lambda t: rank[t.name]):
            if t.name not in sent and all(d in seen for d in t.deps):
                if free.get(t.link, 0.0) - now > depth:
                    continue
                free[t.link] = max(now, free.get(t.link, 0.0)) + cost(t)
                arrive[t.name] = free[t.link] + delay(t)
                sent.add(t.name)
                order.append(("send", t.name))

    order.append(("load", None))
    seen.add("load")
    issue()
    todo = list(units)
    while todo or len(seen) <= len(transfers):
        waiting = sorted((when, name) for name, when in arrive.items() if name not in seen)
        unit = next((u for u in todo if all(d in seen for d in u[1])), None)
        if waiting and (waiting[0][0] <= now or unit is None):
            when, name = waiting[0]
            if when > now + 0.5 and any(t.name not in sent and all(d in seen for d in t.deps) for t in transfers):
                now += 0.5
                issue()
                continue
            now = max(now, when)
            seen.add(name)
            order.append(("wait", name))
            issue()
        elif unit is not None:
            todo.remove(unit)
            order.append(("head", unit[0]))
            now += unit[2]
            issue()
        else:
            now += 0.2
            issue()
    return order, now, max(arrive.values(), default=0.0)


def kernel(order, index, parts, q_ref, lat_ref, rope_ref, kw_ref, vw_ref, len_ref, out_ref,
           wbuf, qb, latb, ropeb, kexts, vbufs, bias, outb,
           send_sem, recv_sem, load_sem, out_sem, give_sem, take_sem):
    me = {a: lax.axis_index(a) for a in "xyz"}
    core = lax.axis_index("c")
    other = 1 - core
    chip = (me["z"] * NY + me["y"]) * NX + me["x"]

    def at(axis, step):
        return lax.rem(me[axis] + step + 2 * SIZES[axis], SIZES[axis])

    def chip_id(step):
        b = lax.rem(chip + step + NX * NY * NZ, NX * NY * NZ)
        return {"z": b // (NY * NX), "y": lax.rem(b // NX, NY), "x": lax.rem(b, NX)}

    def device(target):
        if target == "core":
            return {"c": other}
        if target == "next":
            return chip_id(1)
        axis, step = target
        return {axis: at(axis, step)}

    barrier = pltpu.get_barrier_semaphore()
    greeted = [{"c": other}, chip_id(1), chip_id(-1)]
    greeted += [{a: at(a, s)} for a in "xyz" for s in range(1, SIZES[a])]
    for d in greeted:
        pl.semaphore_signal(barrier, inc=1, device_id=d, device_id_type=pl.DeviceIdType.MESH)

    loads = []

    def load(src, dst):
        c = pltpu.make_async_copy(src, dst, load_sem.at[len(loads)])
        c.start()
        loads.append(c)

    for h in range(HEADS_EACH):
        for part, ref in enumerate((kw_ref, vw_ref)):
            load(ref.at[:, pl.ds(h * NOPE, NOPE)],
                 wbuf.at[me["x"], h, me["z"], me["y"], :, pl.ds(part * NOPE, NOPE)])
    early = len(loads)
    load(lat_ref, latb.at[4 + core])
    load(rope_ref, ropeb.at[4 + core])
    for x in range(NX):
        start = pl.multiple_of((2 * x + core) * 4 * PAIR, 128)
        load(q_ref.at[:, pl.ds(start, 4 * PAIR)], qb.at[x, core])

    def weight_spot(where):
        spot, heads = where
        idx = {}
        for axis in "xyz":
            what = spot[axis]
            idx[axis] = at(axis, what[1]) if what[0] == "at" else pl.ds(what[0], what[1])
        return wbuf.at[idx["x"], pl.ds(heads[0], heads[1]), idx["z"], idx["y"]]

    def copies(name):
        t = parts[name]
        k = index[name]
        if t.kind == "w":
            pairs = [(weight_spot(t.where), weight_spot(t.where))]
        elif t.kind == "lat":
            src, dst = t.where
            if src == "in":
                pairs = [(lat_ref, latb.at[dst + core]), (rope_ref, ropeb.at[dst + core])]
            else:
                pairs = [(latb.at[src + core], latb.at[dst + core]),
                         (ropeb.at[src + core], ropeb.at[dst + core])]
        else:
            start = pl.multiple_of((2 * t.where + other) * 4 * PAIR, 128)
            pairs = [(q_ref.at[:, pl.ds(start, 4 * PAIR)], qb.at[t.where, core])]
        return [
            pltpu.make_async_remote_copy(
                src_ref=s, dst_ref=d, send_sem=send_sem.at[k + i], recv_sem=recv_sem.at[k + i],
                device_id=device(t.target), device_id_type=pl.DeviceIdType.MESH,
            )
            for i, (s, d) in enumerate(pairs)
        ]

    lane = lax.broadcasted_iota(jnp.int32, (TOK, 128), 1)

    def make_bias():
        lens = len_ref[...].astype(jnp.float32)
        rows = lax.broadcasted_iota(jnp.int32, (128, 128), 0)
        cols = lax.broadcasted_iota(jnp.int32, (128, 128), 1)
        as_rows = jnp.broadcast_to(lens, (128, 128))
        starts = jnp.sum(jnp.where(cols < rows, as_rows, 0.0), axis=1, keepdims=True)
        for half in range(NC):
            base = chip * (NC * TOK) + half * TOK
            q_pos = (base + cols).astype(jnp.float32)
            started = jnp.where(starts <= q_pos, starts, 0.0)
            q_start = jnp.max(started, axis=0, keepdims=True)
            k_pos = (base - 4 * TOK + lax.broadcasted_iota(jnp.int32, (WIN, TOK), 0)).astype(jnp.float32)
            q_row = (base + lax.broadcasted_iota(jnp.int32, (WIN, TOK), 1)).astype(jnp.float32)
            bias[half] = jnp.where((k_pos >= q_start) & (k_pos <= q_row), 0.0, LOWEST)

    def prepare():
        for s in range(6):
            r = ropeb[s].astype(jnp.float32)
            r = jnp.transpose(jnp.concatenate([r, r], axis=0))
            spot = pl.ds(s * TOK, TOK)
            low = lane < ROPE
            for slot in range(4):
                kexts[2 * slot, spot, NOPE:] = jnp.where(low, r, 0.0).astype(jnp.bfloat16)
                kexts[2 * slot + 1, spot, :NOPE] = jnp.where(low, 0.0, r).astype(jnp.bfloat16)
        for slot in range(4):
            vbufs[slot, :, VDIM:] = jnp.ones((KEYS, VDIM), jnp.bfloat16)

        def order_queries(i, carry):
            x, half = i // NC, lax.rem(i, NC)
            for pair in range(HEADS_EACH // 2):
                mid = qb[x, half, :, pl.ds(pair * PAIR + 128, 128)].astype(jnp.float32)
                end = qb[x, half, :, pl.ds(pair * PAIR + 256, 128)].astype(jnp.float32)
                low = lane < ROPE
                qb[x, half, :, pl.ds(pair * PAIR + 128, 128)] = jnp.where(low, mid, end).astype(jnp.bfloat16)
                turned = pltpu.roll(jnp.where(low, end, mid), ROPE, 1)
                qb[x, half, :, pl.ds(pair * PAIR + 256, 128)] = turned.astype(jnp.bfloat16)
            return carry

        lax.fori_loop(0, NX * NC, order_queries, 0)

    def project(x, h, slot):
        w = wbuf[x, h].reshape(LATENT, 2 * NOPE)
        kv = jnp.dot(latb[...].reshape(KEYS, LATENT), w, preferred_element_type=jnp.float32)
        vbufs[slot, :, :VDIM] = kv[:, NOPE:].astype(jnp.bfloat16)
        place = slice(NOPE, 2 * NOPE) if h % 2 else slice(0, NOPE)
        kexts[2 * slot + h % 2, :, place] = kv[:, :NOPE].astype(jnp.bfloat16)

    def attend(x, h, slot):
        column = (h // 2) * PAIR + (h % 2) * 128
        q = qb[x, :, :, pl.ds(column, 256)].reshape(NC * TOK, 256)
        scores = lax.dot_general(kexts[2 * slot + h % 2], q, NT, preferred_element_type=jnp.float32)
        for half in range(NC):
            at_keys, at_rows = slice(half * TOK, half * TOK + WIN), slice(half * TOK, half * TOK + TOK)
            s = scores[at_keys, at_rows] + bias[half]
            peak = jnp.max(s, axis=0, keepdims=True)
            expo = jnp.exp2((s - peak) * EXP_SCALE)
            mixed = lax.dot_general(expo.astype(jnp.bfloat16), vbufs[slot, at_keys, :], TN,
                                    preferred_element_type=jnp.float32)
            outb[half, x, h] = (mixed[:, :VDIM] / mixed[:, VDIM:]).astype(jnp.bfloat16)

    def heads_of(xs, h):
        for slot, x in enumerate(xs):
            project(x, h, slot)
        for slot, x in enumerate(xs):
            attend(x, h, slot)

    def out_copies(x, h):
        mine = pl.multiple_of(((2 * x + core) * HEADS_EACH + h) * VDIM, VDIM)
        slot = x * HEADS_EACH + h
        spot = out_ref.at[:, pl.ds(mine, VDIM)]
        local = pltpu.make_async_copy(outb.at[core, x, h], spot, out_sem.at[slot])
        away = pltpu.make_async_remote_copy(
            src_ref=outb.at[other, x, h], dst_ref=spot,
            send_sem=give_sem.at[slot], recv_sem=take_sem.at[slot],
            device_id={"c": other}, device_id_type=pl.DeviceIdType.MESH,
        )
        return local, away

    def put_out(done):
        for x, h in done:
            for c in out_copies(x, h):
                c.start()

    pl.semaphore_wait(barrier, len(greeted))
    sent, finished, state = [], [], set()
    for what, name in order:
        if what == "load":
            for c in loads[:early]:
                c.wait()
        elif what == "send":
            for c in copies(name):
                c.start()
            sent.append(name)
        elif what == "wait":
            if "bias" not in state:
                make_bias()
                state.add("bias")
            for c in copies(name):
                c.wait_recv()
        elif what == "head":
            if "prepared" not in state:
                for c in loads[early:]:
                    c.wait()
                prepare()
                state.add("prepared")
            kind, h, steps = name
            if kind == "a":
                xs = [at("x", dx) for dx in steps]
                heads_of(xs, h)
            else:
                xs = list(range(NX))
                heads_of(xs, h)
            put_out(finished)
            finished = [(x, h) for x in xs]
    put_out(finished)
    for name in sent:
        for c in copies(name):
            c.wait_send()
    for x in range(NX):
        for h in range(HEADS_EACH):
            local, away = out_copies(x, h)
            local.wait()
            away.wait()


def shards(queries, latent, rope_keys, key_weight, value_weight, doc_lengths):
    weights, ready = weight_transfers()
    rest, lat_names = other_transfers()
    transfers = weights + rest
    after = lat_names + [t.name for t in rest if t.kind == "q"] + ["load"]
    units = [(k, v + after, UNIT_US[NX if k[2] is None else len(k[2])]) for k, v in ready.items()]
    order = plan(transfers, units, depth=DEPTH)[0]
    index, at = {}, 0
    for t in transfers:
        index[t.name] = at
        at += 2 if t.kind == "lat" else 1
    parts = {t.name: t for t in transfers}
    hbm = pl.BlockSpec(memory_space=pl.ANY)
    bf = jnp.bfloat16
    return pl.pallas_call(
        functools.partial(kernel, order, index, parts),
        out_shape=jax.ShapeDtypeStruct((TOK, 64 * VDIM), bf),
        in_specs=[hbm] * 5 + [pl.BlockSpec(memory_space=pltpu.VMEM)],
        out_specs=hbm,
        scratch_shapes=[
            pltpu.VMEM((NX, HEADS_EACH, NZ, NY, SLAB, 2 * NOPE), bf),
            pltpu.VMEM((NX, NC, TOK, 4 * PAIR), bf),
            pltpu.VMEM((6, TOK, LATENT), bf),
            pltpu.VMEM((6, ROPE, TOK), bf),
            pltpu.VMEM((8, KEYS, 256), bf),
            pltpu.VMEM((4, KEYS, 2 * VDIM), bf),
            pltpu.VMEM((NC, WIN, TOK), jnp.float32),
            pltpu.VMEM((NC, NX, HEADS_EACH, TOK, VDIM), bf),
            pltpu.SemaphoreType.DMA((at,)),
            pltpu.SemaphoreType.DMA((at,)),
            pltpu.SemaphoreType.DMA((2 * HEADS_EACH + 2 + NX,)),
            pltpu.SemaphoreType.DMA((NX * HEADS_EACH,)),
            pltpu.SemaphoreType.DMA((NX * HEADS_EACH,)),
            pltpu.SemaphoreType.DMA((NX * HEADS_EACH,)),
        ],
        compiler_params=pltpu.CompilerParams(
            collective_id=0, has_side_effects=True, vmem_limit_bytes=56 * 2**20
        ),
    )(queries, latent, rope_keys.T, key_weight, value_weight, doc_lengths.reshape(1, -1))


def solution(mesh):
    torus = Mesh(mesh.devices.reshape(NZ, NY, NX, NC), ("z", "y", "x", "c"))
    rows = P(("z", "y", "x", "c"), None)
    weight = P(("z", "y"), ("x", "c"))
    return jax.shard_map(
        shards, mesh=torus, in_specs=(rows, rows, rows, weight, weight, P()), out_specs=rows,
        check_vma=False,
    )
```

```python
import functools
import math

import jax
import jax.numpy as jnp
from jax import lax
from jax.experimental import pallas as pl
from jax.experimental.pallas import tpu as pltpu
from jax.sharding import Mesh
from jax.sharding import PartitionSpec as P

NOPE = 128
ROPE = 64
VDIM = 128
PAIR = 384
NX, NY, NZ, NC = 4, 4, 8, 2
HEADS_EACH = 8
SLAB = 16
TOK = 128
KEYS = 6 * TOK
WIN = 5 * TOK
LATENT = 512
LOWEST = -1e30
EXP_SCALE = math.log2(math.e) / math.sqrt(NOPE + ROPE)
SIZES = {"x": NX, "y": NY, "z": NZ}
FULL = {"x": (0, NX), "y": (0, NY), "z": (0, NZ)}

FIRST = [
    ('b', (4, 1), 'x', 'direct', 1),
    ('a', (0, 1), 'z', 'direct', 1),
    ('B', (5, 1), 'z', 'direct', -1),
    ('c', (6, 2), 'x', 'direct', -1),
    ('l', (1, 3), 'z', 'ring', 1),
]
CHAINS = [
    ('a0', 'a', (0, 1), 'zyx', True, ('z', 'z'), 3),
    ('b0', 'B', (5, 1), 'zxy', True, ('z', 'z'), None),
    ('c', 'c', (6, 1), 'xyz', False, ('x', 'x'), None),
    ('d', 'c', (7, 1), 'xyz', False, ('x', 'x'), None),
    ('a1', 'l', (1, 1), 'zyx', False, ('z', 'z'), 3),
    ('b1', 'b', (4, 1), 'xzy', False, ('x', 'x'), None),
    ('a2', 'l', (2, 1), 'zyx', True, ('z', 'z'), 3),
    ('b2', 'l', (3, 1), 'zxy', False, ('z', 'z'), None),
]
DEPTH = 8.0
LATE = 0.0
FIXED_US = 1.4
HOP_US = 0.9
UNIT_US = {1: 1.15, 2: 1.55, 4: 2.6}
NT = (((1,), (1,)), ((), ()))
TN = (((0,), (0,)), ((), ()))


ORDER = {"fb": -19.4, "fa": -6.0, "fB": -14.9, "fc": -20.8, "fl": -6.7, "a0": -4.4, "a0h0": -0.6, "b0": -5.2, "b0h5": 17.1, "c": 2.0, "ch6": 0.9, "d": 2.7, "dh7": 15.9, "a1": -11.2, "a1h1": 24.8, "b1": -1.6, "b1h4": 10.0, "a2": -19.8, "a2h2": 3.3, "b2": -14.1, "b2h3": 22.7, "lat": -19.1, "q": 9.6}
REACH_SHARE = 0.6


def stage(name):
    if name[0] == "f":
        return name[:2]
    if name[0] in "lq":
        return "lat" if name[0] == "l" else "q"
    return name[:name.index("u")] if "u" in name else name[:-3]


def PRIORITY(t, reach):
    return ORDER[stage(t.name)] - REACH_SHARE * reach


class Transfer:
    def __init__(self, name, kind, where, target, deps, link, size, hops=1, late=0.0):
        self.name, self.kind, self.where, self.target = name, kind, where, target
        self.deps, self.link, self.size, self.hops, self.late = list(deps), link, size, hops, late


def weight_transfers():
    out, ready = [], {}

    def own(**over):
        spot = {"x": ("at", 0), "y": ("at", 0), "z": ("at", 0)}
        spot.update(over)
        return spot

    def add(name, spot, heads, target, deps, hops=1):
        axis, step = target
        count = heads[1]
        for a in "xyz":
            count *= 1 if spot[a][0] == "at" else spot[a][1]
        link = axis + ("+" if step > 0 else "-")
        size = count * SLAB * 2 * NOPE * 2
        out.append(Transfer(name, "w", (spot, heads), target, deps, link, size, hops))
        return name

    def direct(tag, axis, heads, deps, far=1):
        n = SIZES[axis]
        steps = [s for d in range(1, n // 2) for s in (d, -d)] + [far * (n // 2)]
        return [add(f"{tag}{axis}{s}", own(), heads, (axis, s), deps, abs(s)) for s in steps]

    def ring(tag, axis, spot, heads, deps, half_axis, forward=None):
        n = SIZES[axis]
        got = {0: list(deps)}
        lo, width = heads if half_axis == "h" else spot.get(half_axis, (0, 2))
        cut = width // 2 if forward is None else forward
        for sign in (1, -1):
            last = list(deps)
            for k in range(1, n // 2 + 1):
                piece, part = dict(spot), heads
                piece[axis] = ("at", -sign * (k - 1))
                if k == n // 2:
                    share = (lo, cut) if sign > 0 else (lo + cut, width - cut)
                    if share[1] == 0:
                        continue
                    if half_axis == "h":
                        part = share
                    elif half_axis:
                        piece[half_axis] = share
                name = add(f"{tag}{axis}{'+' if sign > 0 else '-'}{k}", piece, part, (axis, sign), last)
                last = [name]
                got.setdefault(n // 2 if k == n // 2 else -sign * k, []).append(name)
        return got

    def last_ring(tag, axis, inner, spot, heads, units, half_axis, forward=None):
        got = {}
        for offset, deps in units.items():
            piece, way = dict(spot), forward
            if offset is None:
                piece[inner] = FULL[inner]
            else:
                piece[inner] = ("at", offset)
            for o, names in ring(f"{tag}u{offset}", axis, piece, heads, deps, half_axis, way).items():
                got.setdefault(o, []).extend(names)
        return {o: sorted(set(names)) for o, names in got.items()}

    def merged(units):
        return {None: sorted(set(sum(units.values(), [])))}

    local = ["load"]
    first = {}
    for tag, heads, axis, how, far in FIRST:
        if how == "direct":
            names = direct(f"f{tag}", axis, heads, local, far)
        else:
            names = sorted(set(sum(ring(f"f{tag}", axis, own(), heads, local, "h").values(), [])))
        first[tag] = names + local
    for tag, source, heads, axes, fine, halves, forward in CHAINS:
        a, b, c = axes
        units = ring(f"{tag}", b, own(**{a: FULL[a]}), heads, first[source], halves[0])
        if not fine:
            units = merged(units)
        for h in range(heads[0], heads[0] + heads[1]):
            got = last_ring(f"{tag}h{h}", c, b, own(**{a: FULL[a]}), (h, 1), units, halves[1], forward)
            if c == "x":
                ready[("a", h, (0,))] = got[0]
                ready[("a", h, (-1, 1))] = sorted(set(got[-1] + got[1]))
                ready[("a", h, (2,))] = got[2]
            else:
                ready[("b", h, None)] = sorted(set(sum(got.values(), [])))
    return out, ready


def other_transfers():
    lat = TOK * (LATENT + 64) * 2
    q = TOK * 4 * PAIR * 2
    out = [
        Transfer("lat.next", "lat", ("in", 2), "next", [], "x+", lat, 1, LATE),
        Transfer("lat.core", "lat", ("in", 4), "core", [], "c", lat),
        Transfer("lat.next2", "lat", (2, 0), "next", ["lat.next"], "x+", lat, 1, LATE),
        Transfer("lat.core1", "lat", (2, 2), "core", ["lat.next"], "c", lat),
        Transfer("lat.core2", "lat", (0, 0), "core", ["lat.next2"], "c", lat),
    ]
    lat_names = [t.name for t in out]
    for x in range(NX):
        out.append(Transfer(f"q{x}", "q", x, "core", [], "c", q))
    return out, lat_names


def plan(transfers, units, rate=45e3, d2d=500e3, depth=4.0):
    by_name = {t.name: t for t in transfers}
    tail, follow = {}, {}
    for t in transfers:
        for d in t.deps:
            follow.setdefault(d, []).append(t.name)

    def cost(t):
        return t.size * t.hops / (d2d if t.link == "c" else rate)

    def delay(t):
        return FIXED_US + HOP_US * t.hops + t.late

    def reach(name):
        if name not in tail:
            tail[name] = cost(by_name[name]) + delay(by_name[name]) + max(
                [reach(f) for f in follow.get(name, [])], default=0.0)
        return tail[name]

    rank = {t.name: (PRIORITY(t, reach(t.name)), i) for i, t in enumerate(transfers)}
    free, arrive, sent = {}, {}, set()
    order, seen = [], set()
    now = 0.0

    def issue():
        for t in sorted(transfers, key=lambda t: rank[t.name]):
            if t.name not in sent and all(d in seen for d in t.deps):
                if free.get(t.link, 0.0) - now > depth:
                    continue
                free[t.link] = max(now, free.get(t.link, 0.0)) + cost(t)
                arrive[t.name] = free[t.link] + delay(t)
                sent.add(t.name)
                order.append(("send", t.name))

    order.append(("load", None))
    seen.add("load")
    issue()
    todo = list(units)
    while todo or len(seen) <= len(transfers):
        waiting = sorted((when, name) for name, when in arrive.items() if name not in seen)
        unit = next((u for u in todo if all(d in seen for d in u[1])), None)
        if waiting and (waiting[0][0] <= now or unit is None):
            when, name = waiting[0]
            if when > now + 0.5 and any(t.name not in sent and all(d in seen for d in t.deps) for t in transfers):
                now += 0.5
                issue()
                continue
            now = max(now, when)
            seen.add(name)
            order.append(("wait", name))
            issue()
        elif unit is not None:
            todo.remove(unit)
            order.append(("head", unit[0]))
            now += unit[2]
            issue()
        else:
            now += 0.2
            issue()
    return order, now, max(arrive.values(), default=0.0)


def kernel(order, index, parts, q_ref, lat_ref, rope_ref, kw_ref, vw_ref, len_ref, out_ref,
           wbuf, qb, latb, ropeb, kexts, vbufs, bias, outb,
           send_sem, recv_sem, load_sem, out_sem, give_sem, take_sem):
    me = {a: lax.axis_index(a) for a in "xyz"}
    core = lax.axis_index("c")
    other = 1 - core
    chip = (me["z"] * NY + me["y"]) * NX + me["x"]

    def at(axis, step):
        return lax.rem(me[axis] + step + 2 * SIZES[axis], SIZES[axis])

    def chip_id(step):
        b = lax.rem(chip + step + NX * NY * NZ, NX * NY * NZ)
        return {"z": b // (NY * NX), "y": lax.rem(b // NX, NY), "x": lax.rem(b, NX)}

    def device(target):
        if target == "core":
            return {"c": other}
        if target == "next":
            return chip_id(1)
        axis, step = target
        return {axis: at(axis, step)}

    barrier = pltpu.get_barrier_semaphore()
    greeted = [{"c": other}, chip_id(1), chip_id(-1)]
    greeted += [{a: at(a, s)} for a in "xyz" for s in range(1, SIZES[a])]
    for d in greeted:
        pl.semaphore_signal(barrier, inc=1, device_id=d, device_id_type=pl.DeviceIdType.MESH)

    loads = []

    def load(src, dst):
        c = pltpu.make_async_copy(src, dst, load_sem.at[len(loads)])
        c.start()
        loads.append(c)

    for h in range(HEADS_EACH):
        for part, ref in enumerate((kw_ref, vw_ref)):
            load(ref.at[:, pl.ds(h * NOPE, NOPE)],
                 wbuf.at[me["x"], h, me["z"], me["y"], :, pl.ds(part * NOPE, NOPE)])
    early = len(loads)
    load(lat_ref, latb.at[4 + core])
    load(rope_ref, ropeb.at[4 + core])
    for x in range(NX):
        start = pl.multiple_of((2 * x + core) * 4 * PAIR, 128)
        load(q_ref.at[:, pl.ds(start, 4 * PAIR)], qb.at[x, core])

    def weight_spot(where):
        spot, heads = where
        idx = {}
        for axis in "xyz":
            what = spot[axis]
            idx[axis] = at(axis, what[1]) if what[0] == "at" else pl.ds(what[0], what[1])
        return wbuf.at[idx["x"], pl.ds(heads[0], heads[1]), idx["z"], idx["y"]]

    def copies(name):
        t = parts[name]
        k = index[name]
        if t.kind == "w":
            pairs = [(weight_spot(t.where), weight_spot(t.where))]
        elif t.kind == "lat":
            src, dst = t.where
            if src == "in":
                pairs = [(lat_ref, latb.at[dst + core]), (rope_ref, ropeb.at[dst + core])]
            else:
                pairs = [(latb.at[src + core], latb.at[dst + core]),
                         (ropeb.at[src + core], ropeb.at[dst + core])]
        else:
            start = pl.multiple_of((2 * t.where + other) * 4 * PAIR, 128)
            pairs = [(q_ref.at[:, pl.ds(start, 4 * PAIR)], qb.at[t.where, core])]
        return [
            pltpu.make_async_remote_copy(
                src_ref=s, dst_ref=d, send_sem=send_sem.at[k + i], recv_sem=recv_sem.at[k + i],
                device_id=device(t.target), device_id_type=pl.DeviceIdType.MESH,
            )
            for i, (s, d) in enumerate(pairs)
        ]

    lane = lax.broadcasted_iota(jnp.int32, (TOK, 128), 1)

    def make_bias():
        lens = len_ref[...].astype(jnp.float32)
        rows = lax.broadcasted_iota(jnp.int32, (128, 128), 0)
        cols = lax.broadcasted_iota(jnp.int32, (128, 128), 1)
        as_rows = jnp.broadcast_to(lens, (128, 128))
        starts = jnp.sum(jnp.where(cols < rows, as_rows, 0.0), axis=1, keepdims=True)
        for half in range(NC):
            base = chip * (NC * TOK) + half * TOK
            q_pos = (base + cols).astype(jnp.float32)
            started = jnp.where(starts <= q_pos, starts, 0.0)
            q_start = jnp.max(started, axis=0, keepdims=True)
            k_pos = (base - 4 * TOK + lax.broadcasted_iota(jnp.int32, (WIN, TOK), 0)).astype(jnp.float32)
            q_row = (base + lax.broadcasted_iota(jnp.int32, (WIN, TOK), 1)).astype(jnp.float32)
            bias[half] = jnp.where((k_pos >= q_start) & (k_pos <= q_row), 0.0, LOWEST)

    low = lane < ROPE

    def make_ones():
        for slot in range(4):
            vbufs[slot, :, VDIM:] = jnp.ones((KEYS, VDIM), jnp.bfloat16)

    def place_rope(s):
        r = ropeb[s].astype(jnp.float32)
        r = jnp.transpose(jnp.concatenate([r, r], axis=0))
        spot = pl.ds(pl.multiple_of(s * TOK, TOK), TOK)
        first = jnp.where(low, r, 0.0).astype(jnp.bfloat16)
        second = jnp.where(low, 0.0, r).astype(jnp.bfloat16)
        for slot in range(4):
            kexts[2 * slot, spot, NOPE:] = first
            kexts[2 * slot + 1, spot, :NOPE] = second

    def order_queries(x, half):
        for pair in range(HEADS_EACH // 2):
            mid = qb[x, half, :, pl.ds(pair * PAIR + 128, 128)].astype(jnp.float32)
            end = qb[x, half, :, pl.ds(pair * PAIR + 256, 128)].astype(jnp.float32)
            qb[x, half, :, pl.ds(pair * PAIR + 128, 128)] = jnp.where(low, mid, end).astype(jnp.bfloat16)
            turned = pltpu.roll(jnp.where(low, end, mid), ROPE, 1)
            qb[x, half, :, pl.ds(pair * PAIR + 256, 128)] = turned.astype(jnp.bfloat16)

    def settle(name):
        if name[0] == "q":
            order_queries(parts[name].where, other)
        elif name[0] == "l":
            place_rope({"lat.core": 4 + other, "lat.next": 2 + core, "lat.core1": 2 + other,
                        "lat.next2": core, "lat.core2": other}[name])

    def project(x, h, slot):
        w = wbuf[x, h].reshape(LATENT, 2 * NOPE)
        kv = jnp.dot(latb[...].reshape(KEYS, LATENT), w, preferred_element_type=jnp.float32)
        vbufs[slot, :, :VDIM] = kv[:, NOPE:].astype(jnp.bfloat16)
        place = slice(NOPE, 2 * NOPE) if h % 2 else slice(0, NOPE)
        kexts[2 * slot + h % 2, :, place] = kv[:, :NOPE].astype(jnp.bfloat16)

    def attend(x, h, slot):
        column = (h // 2) * PAIR + (h % 2) * 128
        q = qb[x, :, :, pl.ds(column, 256)].reshape(NC * TOK, 256)
        scores = lax.dot_general(kexts[2 * slot + h % 2], q, NT, preferred_element_type=jnp.float32)
        for half in range(NC):
            at_keys, at_rows = slice(half * TOK, half * TOK + WIN), slice(half * TOK, half * TOK + TOK)
            s = scores[at_keys, at_rows] + bias[half]
            peak = jnp.max(s, axis=0, keepdims=True)
            expo = jnp.exp2((s - peak) * EXP_SCALE)
            mixed = lax.dot_general(expo.astype(jnp.bfloat16), vbufs[slot, at_keys, :], TN,
                                    preferred_element_type=jnp.float32)
            outb[half, x, h] = (mixed[:, :VDIM] / mixed[:, VDIM:]).astype(jnp.bfloat16)

    def heads_of(xs, h):
        for slot, x in enumerate(xs):
            project(x, h, slot)
        for slot, x in enumerate(xs):
            attend(x, h, slot)

    def out_copies(x, h):
        mine = pl.multiple_of(((2 * x + core) * HEADS_EACH + h) * VDIM, VDIM)
        slot = x * HEADS_EACH + h
        spot = out_ref.at[:, pl.ds(mine, VDIM)]
        local = pltpu.make_async_copy(outb.at[core, x, h], spot, out_sem.at[slot])
        away = pltpu.make_async_remote_copy(
            src_ref=outb.at[other, x, h], dst_ref=spot,
            send_sem=give_sem.at[slot], recv_sem=take_sem.at[slot],
            device_id={"c": other}, device_id_type=pl.DeviceIdType.MESH,
        )
        return local, away

    def put_out(done):
        for x, h in done:
            for c in out_copies(x, h):
                c.start()

    pl.semaphore_wait(barrier, len(greeted))
    sent, finished, arrived, state = [], [], [], set()
    for what, name in order:
        if what != "send":
            while arrived:
                settle(arrived.pop())
        if what == "load":
            for c in loads[:early]:
                c.wait()
        elif what == "send":
            for c in copies(name):
                c.start()
            sent.append(name)
        elif what == "wait":
            if "own" not in state:
                make_bias()
                make_ones()
                for c in loads[early:]:
                    c.wait()
                place_rope(4 + core)
                for x in range(NX):
                    order_queries(x, core)
                state.add("own")
            for c in copies(name):
                c.wait_recv()
            arrived.append(name)
        elif what == "head":
            kind, h, steps = name
            if kind == "a":
                xs = [at("x", dx) for dx in steps]
                heads_of(xs, h)
            else:
                xs = list(range(NX))
                heads_of(xs, h)
            put_out(finished)
            finished = [(x, h) for x in xs]
    put_out(finished)
    for name in sent:
        for c in copies(name):
            c.wait_send()
    for x in range(NX):
        for h in range(HEADS_EACH):
            local, away = out_copies(x, h)
            local.wait()
            away.wait()


def shards(queries, latent, rope_keys, key_weight, value_weight, doc_lengths):
    weights, ready = weight_transfers()
    rest, lat_names = other_transfers()
    transfers = weights + rest
    after = lat_names + [t.name for t in rest if t.kind == "q"] + ["load"]
    units = [(k, v + after, UNIT_US[NX if k[2] is None else len(k[2])]) for k, v in ready.items()]
    order = plan(transfers, units, depth=DEPTH)[0]
    index, at = {}, 0
    for t in transfers:
        index[t.name] = at
        at += 2 if t.kind == "lat" else 1
    parts = {t.name: t for t in transfers}
    hbm = pl.BlockSpec(memory_space=pl.ANY)
    bf = jnp.bfloat16
    return pl.pallas_call(
        functools.partial(kernel, order, index, parts),
        out_shape=jax.ShapeDtypeStruct((TOK, 64 * VDIM), bf),
        in_specs=[hbm] * 5 + [pl.BlockSpec(memory_space=pltpu.VMEM)],
        out_specs=hbm,
        scratch_shapes=[
            pltpu.VMEM((NX, HEADS_EACH, NZ, NY, SLAB, 2 * NOPE), bf),
            pltpu.VMEM((NX, NC, TOK, 4 * PAIR), bf),
            pltpu.VMEM((6, TOK, LATENT), bf),
            pltpu.VMEM((6, ROPE, TOK), bf),
            pltpu.VMEM((8, KEYS, 256), bf),
            pltpu.VMEM((4, KEYS, 2 * VDIM), bf),
            pltpu.VMEM((NC, WIN, TOK), jnp.float32),
            pltpu.VMEM((NC, NX, HEADS_EACH, TOK, VDIM), bf),
            pltpu.SemaphoreType.DMA((at,)),
            pltpu.SemaphoreType.DMA((at,)),
            pltpu.SemaphoreType.DMA((2 * HEADS_EACH + 2 + NX,)),
            pltpu.SemaphoreType.DMA((NX * HEADS_EACH,)),
            pltpu.SemaphoreType.DMA((NX * HEADS_EACH,)),
            pltpu.SemaphoreType.DMA((NX * HEADS_EACH,)),
        ],
        compiler_params=pltpu.CompilerParams(
            collective_id=0, has_side_effects=True, vmem_limit_bytes=56 * 2**20
        ),
    )(queries, latent, rope_keys.T, key_weight, value_weight, doc_lengths.reshape(1, -1))


def solution(mesh):
    torus = Mesh(mesh.devices.reshape(NZ, NY, NX, NC), ("z", "y", "x", "c"))
    rows = P(("z", "y", "x", "c"), None)
    weight = P(("z", "y"), ("x", "c"))
    return jax.shard_map(
        shards, mesh=torus, in_specs=(rows, rows, rows, weight, weight, P()), out_specs=rows,
        check_vma=False,
    )
```
